512 devices in a mesh: group: 2 (over y), ctx: 32 (over z), head: 4 (over x), dec: 2 (over core).
Axes of the slice: x: 4, y: 2, z: 32, core: 2. Of those that a mesh axis runs over, the one named last changes fastest.
The devices are a block of a 4x8x32 slice.
Arguments:
- queries: bfloat16 [8192, 12288], P(('group', 'ctx'), ('head', 'dec')), parts along dimension 0, may hold values from -1100 to 1100
- latent_rows: bfloat16 [8192, 576], P(('group', 'ctx')), parts along dimension 0, may hold values from -8 to 8
- segments: int32 [8192], P('group'), parts along dimension 0, may hold values from 0 to 3, never falling along the last dimension, each value on 1 to 2048 neighbouring positions
- owners: int32 [8192, 1], P(('group', 'ctx')), parts along dimension 0, may hold values from 0 to 63; in each aligned block of 128 rows (0 to 127, 128 to 255, ...) at most 4 rows name the same one
- absorb_key: bfloat16 [64, 128, 512], P(('head', 'dec')), may hold values from -0.5 to 0.5
- absorb_value: bfloat16 [64, 512, 128], P(('head', 'dec')), may hold values from -0.25 to 0.25
Outputs:
- attended: bfloat16 [8192, 8192], P(('group', 'ctx'), ('head', 'dec')), parts along dimension 0
- kv_cache: bfloat16 [128, 32, 4, 576], P(('group', 'ctx', 'dec')), parts along dimension 0
The draws below stay inside these ranges and needn't reach their ends.
There are 2 independent parts, one for each index of `group`. The reference program is written for one: setup_inputs(seed, part) draws one part's arguments, and reference() takes and returns one part's arrays. A program takes and returns all parts, laid end to end along the dimension named above; an argument that names none is the same for every part. Nothing has to cross between parts.
Inputs may be any that keep to these rules, and one draw needn't show every extreme that they name: `segments`: prompt numbers never fall along the tokens; each prompt has 1 to 2048 tokens and one has exactly 2048. `owners`: among the 128 tokens of one index of ctx no owner is named more than 4 times; some owner is named exactly 4 times in some of them; every owner is named somewhere.
All inputs are finite; a program needn't handle non-finite values.
Results may differ from the reference program's by a relative error of at most 0.0085.
Values may be sent and summed in bfloat16 or wider, within the bound.
No kernel may reach another device: no remote copies, remote signals or barrier semaphores. Data moves between devices by JAX's collectives and lax.ppermute only.
A program may use at most 128 MiB of HBM per device.

```python
import math
import jax
import jax.numpy as jnp
import numpy as np
from jax import lax

NOPE = 128
ROPE = 64
LATENT = 512
VDIM = 128
HEADS = 64
DOCS = 4
TOK_DEV = 128
TOKENS = 4096
OWNERS = 64
SLOT = 4
N_CTX = 32


def base_values(key, shape):
    return jnp.clip(jax.random.normal(key, shape, jnp.float32), -6.0, 6.0)


def shared_values(key):
    base_key = jax.random.fold_in(key, 7)
    split_keys = jax.random.split(base_key, 2)
    latent = base_values(split_keys[0], (TOKENS, LATENT + ROPE))
    query = base_values(split_keys[1], (TOKENS, HEADS, NOPE + ROPE))
    return (latent, query.reshape(TOKENS, HEADS * (NOPE + ROPE)))


def draw_queries(key, part):
    return shared_values(key)[1].astype(jnp.bfloat16)


def draw_latent_rows(key, part):
    return shared_values(key)[0].astype(jnp.bfloat16)


def shard_levels(own_key, dims, cuts, low, high):
    level, own = 1.0, jax.random.fold_in(own_key, 6)
    for position, parts in cuts:
        heights = jnp.exp(jax.random.uniform(jax.random.fold_in(own, position), (parts,), jnp.float32, low / len(cuts), high / len(cuts)))
        level = level * jnp.repeat(heights, dims[position] // parts).reshape([-1 if axis == position else 1 for axis in range(len(dims))])
    return level


def profile(amount, total, bound, skew):
    weights = [(1 << 20) // math.isqrt(grade ** skew) + 1 for grade in range(2, amount + 1)]
    rest, given = total - bound - (amount - 1), [1] * (amount - 1)
    while rest > 0:
        free = [i for i in range(amount - 1) if given[i] < bound]
        whole, budget = sum([weights[i] for i in free]), rest
        for i in free:
            more = min(bound - given[i], max(1, budget * weights[i] // whole), rest)
            given[i] = given[i] + more
            rest = rest - more
    return np.array([bound] + given)


def ragged(key, number_of, total, most, slope):
    if number_of == 2:
        one = jax.random.randint(key, (), max(1, total - most), min(most, total - 1) + 1)
        return jnp.stack([one, total - one])
    sizes = jnp.asarray(profile(number_of, total, most, slope), jnp.int32)
    pairs = (number_of - 1) // 2
    source_of, receiver = sizes[1:1 + 2 * pairs:2], sizes[2:2 + 2 * pairs:2]
    margin = jnp.minimum(source_of - 1, most - receiver)
    passed = jax.random.randint(jax.random.fold_in(key, 1), (pairs,), 0, 1 << 20) % (margin + 1)
    sizes = sizes.at[1:1 + 2 * pairs:2].set(source_of - passed).at[2:2 + 2 * pairs:2].set(receiver + passed)
    return sizes[jax.random.permutation(jax.random.fold_in(key, 2), number_of)]


def deal_out(key, own, number, rows, count, top, bound, slope):
    sequence = jax.random.permutation(key, count)
    heavy_load, usual = shares(count, rows * top, bound, slope, True), shares(count, rows * top, bound, slope, False)
    places = jnp.arange(count)

    def named(tallies, rotation):
        used = int((tallies > 0).sum())
        fixed = max(1, used // 4)
        shifted = fixed + (places - fixed + rotation * (used - fixed)) % max(1, count - fixed)
        return jnp.zeros((count,), jnp.int32).at[sequence[jnp.where(places < fixed, places, shifted)]].set(jnp.asarray(tallies, jnp.int32))

    tallies = jnp.where(number % 4 == 0, named(heavy_load, number // 4), named(usual, number - number // 4 - 1))
    mixed = jax.random.permutation(jax.random.fold_in(own, 3), count)
    source_of, receiver = mixed[0:count // 2 * 2:2], mixed[1:count // 2 * 2:2]
    margin = jnp.minimum(tallies[source_of] - 1, bound - tallies[receiver]) // 2
    margin = jnp.where((source_of == sequence[0]) | (receiver == sequence[0]) | (tallies[receiver] == 0), 0, jnp.maximum(margin, 0))
    shifted = jax.random.randint(jax.random.fold_in(own, 4), (count // 2,), 0, 1 << 20) % (margin + 1)
    tallies = tallies.at[source_of].add(-shifted).at[receiver].add(shifted)
    members = jnp.searchsorted(jnp.cumsum(tallies), jnp.arange(rows * top), side="right").astype(jnp.int32)
    table = members.reshape(top, rows).T
    table = table[jax.random.permutation(jax.random.fold_in(own, 1), rows)]
    rotation = jax.random.randint(jax.random.fold_in(own, 2), (rows, 1), 0, top)
    return jnp.take_along_axis(table, (jnp.arange(top)[None, :] + rotation) % top, axis=1)


def shares(number_of, total, bound, skew, full):
    loads = [(1 << 20) // math.isqrt(standing ** skew) + 1 for standing in range(1, number_of + 1)]
    largest = bound if full else min(bound, max(-(-total // number_of), total * loads[0] // sum(loads)))
    least = 1 if total - largest >= number_of - 1 else 0
    counts, spare = [largest] + [least] * (number_of - 1), total - largest - least * (number_of - 1)
    while spare > 0:
        candidates = [i for i in range(1, number_of) if counts[i] < largest] or [i for i in range(1, number_of) if counts[i] < bound]
        pool, remaining = sum([loads[i] for i in candidates]), spare
        for i in candidates:
            extra = min(bound - counts[i], max(1, remaining * loads[i] // pool), spare)
            counts[i] = counts[i] + extra
            spare = spare - extra
    return np.array(counts)


def centred(rng, dims, deviation, most, pieces=(), kind=jnp.bfloat16):
    drawn = deviation * jax.random.normal(rng, dims, jnp.float32)
    if pieces:
        drawn = drawn * shard_levels(rng, dims, pieces, -0.22, 0.18)
    return jnp.clip(drawn, -most, most).astype(kind)


def setup_inputs(seed: int = 0, part: int = 0) -> dict:
    arg_keys = jax.random.split(jax.random.key(seed), 7)
    part_keys = jax.random.split(jax.random.fold_in(arg_keys[6], part), 7)
    queries = draw_queries(jax.random.fold_in(jax.random.fold_in(arg_keys[6], part), 71), part)
    latent_rows = draw_latent_rows(jax.random.fold_in(jax.random.fold_in(arg_keys[6], part), 71), part)
    segments = jnp.searchsorted(jnp.cumsum(ragged(part_keys[2], DOCS, TOKENS, TOKENS // 2, 2)), jnp.arange(TOKENS), side="right").astype(jnp.int32)
    owners_keys = jax.random.split(jax.random.fold_in(part_keys[3], 1), TOKENS // TOK_DEV)
    owners_turns = jax.random.permutation(jax.random.fold_in(part_keys[3], 3), TOKENS // TOK_DEV)
    owners = jax.vmap(lambda own, number: deal_out(jax.random.fold_in(part_keys[3], 2), own, number, TOK_DEV, OWNERS, 1, SLOT, 2))(owners_keys, owners_turns).reshape((TOKENS, 1))
    absorb_key = centred(arg_keys[4], (HEADS, NOPE, LATENT), NOPE ** -0.5, 0.5, ((0, 8),))
    absorb_value = centred(arg_keys[5], (HEADS, LATENT, VDIM), LATENT ** -0.5, 0.25, ((0, 8),))
    return {"queries": queries, "latent_rows": latent_rows, "segments": segments, "owners": owners, "absorb_key": absorb_key, "absorb_value": absorb_value}


def rotate_pairs(rope_part, positions):
    half_rope = ROPE // 2
    frequency = 10000.0 ** (-jnp.arange(half_rope, dtype=jnp.float32) * 2.0 / ROPE)
    angles = positions.astype(jnp.float32)[:, None] * frequency[None, :]
    cosine = jnp.cos(angles)[:, None, :]
    sine_part = jnp.sin(angles)[:, None, :]
    first_part = rope_part[..., :half_rope]
    second = rope_part[..., half_rope:]
    return jnp.concatenate([first_part * cosine - second * sine_part, first_part * sine_part + second * cosine], axis=-1)


def reference(queries, latent_rows, segments, owners, absorb_key, absorb_value):
    width = LATENT + ROPE
    shaped = queries.reshape(TOKENS, HEADS, NOPE + ROPE)
    positions = jnp.arange(TOKENS, dtype=jnp.int32)
    rotated = rotate_pairs(shaped[..., NOPE:].astype(jnp.float32), positions).astype(jnp.bfloat16)
    absorbed = jnp.einsum("thn,hnc->thc", shaped[..., :NOPE].astype(jnp.float32), absorb_key.astype(jnp.float32)).astype(jnp.bfloat16)
    full_query = jnp.concatenate([absorbed, rotated], axis=-1)
    key_rows = latent_rows.astype(jnp.float32)
    values = key_rows[:, :LATENT]
    scale = (NOPE + ROPE) ** -0.5
    allowed = (positions[None, :] <= positions[:, None]) & (segments[None, :] == segments[:, None])

    def one_head(pair):
        query_head, value_map = pair
        scores = jnp.dot(query_head.astype(jnp.float32), key_rows.T, preferred_element_type=jnp.float32) * scale
        masked = jnp.where(allowed, scores, -1e30)
        row_max = jnp.max(masked, axis=1, keepdims=True)
        weights = jnp.where(allowed, jnp.exp(masked - row_max), 0.0)
        sums = jnp.sum(weights, axis=1, keepdims=True)
        mixed = jnp.dot(weights.astype(jnp.bfloat16).astype(jnp.float32), values, preferred_element_type=jnp.float32)
        latent_out = (mixed / sums).astype(jnp.bfloat16)
        return jnp.dot(latent_out.astype(jnp.float32), value_map.astype(jnp.float32), preferred_element_type=jnp.float32).astype(jnp.bfloat16)

    per_head = lax.map(one_head, (jnp.transpose(full_query, (1, 0, 2)), absorb_value))
    attended = jnp.transpose(per_head, (1, 0, 2)).reshape(TOKENS, HEADS * VDIM)

    owner_blocks = owners[:, 0].reshape(N_CTX, TOK_DEV)
    row_order = jnp.arange(TOK_DEV, dtype=jnp.int32)
    earlier = row_order[None, :] < row_order[:, None]
    same_owner = owner_blocks[:, :, None] == owner_blocks[:, None, :]
    slot_rank = jnp.sum(same_owner & earlier[None], axis=2).astype(jnp.int32)
    source = jnp.broadcast_to(jnp.arange(N_CTX, dtype=jnp.int32)[:, None], (N_CTX, TOK_DEV))
    kv_cache = jnp.zeros((OWNERS, N_CTX, SLOT, width), jnp.bfloat16)
    kv_cache = kv_cache.at[owner_blocks.reshape(-1), source.reshape(-1), slot_rank.reshape(-1)].set(latent_rows)
    return attended, kv_cache
```

```python
import jax
import jax.numpy as jnp
from jax import lax
from jax.experimental import pallas as pl
from jax.experimental.pallas import tpu as pltpu
from jax.sharding import PartitionSpec as P

NOPE = 128
ROPE = 64
LATENT = 512
VDIM = 128
WIDTH = LATENT + ROPE
HEAD_IN = NOPE + ROPE
PROMPT = 2048
NEG = -1e30
LOG2E = 1.4426950408889634
EVEN = (2, 10, 6, 14, 8, 4, 12)
ODD = (1, 9, 5, 13, 3, 11, 7, 15, 16)


def query_kernel(ctx_ref, q_ref, ak_ref, cos_ref, sin_ref, seg_ref, fq_ref, start_ref):
    heads = ak_ref.shape[0]
    rows = q_ref.shape[0]
    cos2 = cos_ref[...]
    sin2 = sin_ref[...]
    half = ROPE // 2
    for h in range(heads):
        piece = q_ref[:, h * HEAD_IN:(h + 1) * HEAD_IN]
        absorbed = jnp.dot(piece[:, :NOPE], ak_ref[h], preferred_element_type=jnp.float32)
        fq_ref[h, :, :LATENT] = absorbed.astype(jnp.bfloat16)
        x = piece[:, NOPE:].astype(jnp.float32)
        swapped = jnp.concatenate([x[:, half:], x[:, :half]], axis=1)
        fq_ref[h, :, LATENT:] = (x * cos2 + swapped * sin2).astype(jnp.bfloat16)
    own = seg_ref[pl.ds(ctx_ref[0], 1), :]
    own = jnp.broadcast_to(own, (rows, rows)).T
    below = jnp.zeros((rows, rows), jnp.int32)
    for b in range(seg_ref.shape[0]):
        below = below + (seg_ref[b:b + 1, :] < own).astype(jnp.int32)
    start = jnp.sum(below, axis=1, keepdims=True)
    start_ref[...] = jnp.broadcast_to(start, (rows, rows))


def pick_kernel(core_ref, owner_ref, latent_ref, out_ref, *, cores, slots):
    rows = latent_ref.shape[0]
    own = jnp.broadcast_to(owner_ref[...], (rows, rows))
    across = own.T
    down_id = lax.broadcasted_iota(jnp.int32, (rows, rows), 0)
    across_id = lax.broadcasted_iota(jnp.int32, (rows, rows), 1)
    hit = ((own == across) & (down_id < across_id)).astype(jnp.int32)
    rank = jnp.sum(hit, axis=0, keepdims=True)
    name = across[:1, :]
    target = name // cores * slots + rank
    target = jnp.where(name % cores == core_ref[0], target, -1)
    slot_id = lax.broadcasted_iota(jnp.int32, (out_ref.shape[0], rows), 0)
    picker = (slot_id == target).astype(jnp.float32).astype(jnp.bfloat16)
    out_ref[...] = jnp.dot(
        picker, latent_ref[...], preferred_element_type=jnp.float32
    ).astype(jnp.bfloat16)


def place(pieces, replicas, keys_ref, count):
    for piece, replica in zip(pieces, replicas):
        for b in range(count):
            at = pl.multiple_of(b * 128 + replica * 16, 16)
            keys_ref[pl.ds(at, 16), :] = piece[b * 16:(b + 1) * 16, :]


def fill_bias(bias_ref, start, ctx, dists, own_block):
    rows = start.shape[0]
    lane = lax.broadcasted_iota(jnp.int32, (rows, rows), 1)
    for b, dist in enumerate(dists):
        pos = (ctx - dist) * rows + lane
        bias_ref[:, b * rows:(b + 1) * rows] = jnp.where(pos >= start, 0.0, NEG)
    if own_block:
        b = len(dists)
        pos = ctx * rows + lane
        down = lax.broadcasted_iota(jnp.int32, (rows, rows), 0)
        bias_ref[:, b * rows:(b + 1) * rows] = jnp.where(
            (pos >= start) & (lane <= down), 0.0, NEG
        )


def score(fq_ref, h, n, keys_ref, bias_ref):
    rows = fq_ref.shape[1]
    q = fq_ref[h:h + n].reshape(n * rows, WIDTH)
    s = lax.dot_general(
        q, keys_ref[...], (((1,), (1,)), ((), ())), preferred_element_type=jnp.float32
    )
    return s.reshape(n, rows, -1) + bias_ref[...][None]


def first_kernel(meta_ref, fq_ref, start_ref, latent_ref, near_ref, far_ref,
                 max_ref, sum_ref, acc_ref, keys_ref, bias_ref, *, scale, group):
    count = len(EVEN)
    heads, rows = fq_ref.shape[0], fq_ref.shape[1]
    piece = count * 16
    for i in range(4):
        place([near_ref[i * piece:(i + 1) * piece, :], far_ref[i * piece:(i + 1) * piece, :]],
              [meta_ref[1 + i], meta_ref[5 + i]], keys_ref, count)
    keys_ref[count * rows:, :] = latent_ref[...]
    fill_bias(bias_ref, start_ref[...], meta_ref[0], EVEN, True)
    factor = scale * LOG2E
    for h in range(0, heads, group):
        s = score(fq_ref, h, group, keys_ref, bias_ref)
        top = jnp.max(s, axis=2, keepdims=True)
        p = jnp.exp2((s - top) * factor)
        total = jnp.sum(p, axis=2, keepdims=True)
        acc = jnp.dot(
            p.astype(jnp.bfloat16).reshape(group * rows, -1), keys_ref[:, :LATENT],
            preferred_element_type=jnp.float32,
        )
        acc_ref[h:h + group] = acc.reshape(group, rows, LATENT)
        max_ref[h:h + group] = jnp.broadcast_to(top, (group, rows, 128))
        sum_ref[h:h + group] = jnp.broadcast_to(total, (group, rows, 128))


def second_kernel(meta_ref, fq_ref, start_ref, max_ref, sum_ref, acc_ref, near_ref, far_ref,
                  av_ref, out_ref, keys_ref, bias_ref, *, scale, group):
    count = len(ODD)
    heads, rows = fq_ref.shape[0], fq_ref.shape[1]
    piece = count * 16
    for i in range(4):
        place([near_ref[i * piece:(i + 1) * piece, :], far_ref[i * piece:(i + 1) * piece, :]],
              [meta_ref[1 + i], meta_ref[5 + i]], keys_ref, count)
    fill_bias(bias_ref, start_ref[...], meta_ref[0], ODD, False)
    factor = scale * LOG2E
    for h in range(0, heads, group):
        s = score(fq_ref, h, group, keys_ref, bias_ref)
        before = max_ref[h:h + group][:, :, :1]
        top = jnp.maximum(before, jnp.max(s, axis=2, keepdims=True))
        p = jnp.exp2((s - top) * factor)
        keep = jnp.exp2((before - top) * factor)
        total = sum_ref[h:h + group][:, :, :1] * keep + jnp.sum(p, axis=2, keepdims=True)
        acc = jnp.dot(
            p.astype(jnp.bfloat16).reshape(group * rows, -1), keys_ref[:, :LATENT],
            preferred_element_type=jnp.float32,
        ).reshape(group, rows, LATENT)
        mixed = (acc + acc_ref[h:h + group] * keep) / total
        mixed = mixed.astype(jnp.bfloat16)
        for g in range(group):
            out_ref[:, (h + g) * VDIM:(h + g + 1) * VDIM] = jnp.dot(
                mixed[g], av_ref[h + g], preferred_element_type=jnp.float32
            ).astype(jnp.bfloat16)


def vmem(n):
    return [pl.BlockSpec(memory_space=pltpu.VMEM) for _ in range(n)]


SMEM = pl.BlockSpec(memory_space=pltpu.SMEM)


def on_device(queries, latent_rows, segments, owners, absorb_key, absorb_value):
    rows = queries.shape[0]
    heads = absorb_key.shape[0]
    ctx_count = lax.axis_size("ctx")
    head_count = lax.axis_size("head")
    dec_count = lax.axis_size("dec")
    ctx = lax.axis_index("ctx")
    head = lax.axis_index("head")
    core = lax.axis_index("dec")
    scale = (NOPE + ROPE) ** (-0.5)
    bf16 = jnp.bfloat16

    slots = max(2, 2 * rows // (ctx_count * dec_count))
    outgoing = pl.pallas_call(
        lambda *refs: pick_kernel(*refs, cores=dec_count, slots=slots),
        out_shape=jax.ShapeDtypeStruct((ctx_count * slots, WIDTH), bf16),
        in_specs=[SMEM] + vmem(2), out_specs=vmem(1)[0], name="pick",
    )(core[None], owners, latent_rows)
    outgoing = outgoing.reshape(ctx_count, slots, WIDTH)
    arrived = lax.all_to_all(outgoing, "ctx", split_axis=0, concat_axis=0, tiled=True)

    replica = head * dec_count + core
    share = rows // (head_count * dec_count)
    own = lax.dynamic_slice_in_dim(latent_rows, replica * share, share, 0)

    def shift(x, k):
        return lax.ppermute(x, "ctx", [(i, i + k) for i in range(ctx_count - k)])

    cat = lambda *xs: jnp.concatenate(xs, axis=0)
    d8 = shift(own, 8)
    d4 = shift(cat(own, d8), 4)
    four = cat(own, d8, d4)
    d2 = shift(four, 2)
    even = cat(d2, d8, d4)
    d1 = shift(cat(own, d8, d4, d2), 1)
    d16 = shift(d2[3 * share:], 2)
    odd = cat(d1, d16)

    def spread(x):
        ring = lambda k: [(i, (i + k) % head_count) for i in range(head_count)]
        near = cat(x, *[lax.ppermute(x, "head", ring(k)) for k in range(1, head_count)])
        far = lax.ppermute(near, "dec", [(i, (i + 1) % dec_count) for i in range(dec_count)])
        return near, far

    near_even, far_even = spread(even)
    near_odd, far_odd = spread(odd)

    half = ROPE // 2
    frequency = 10000.0 ** (-jnp.arange(half, dtype=jnp.float32) * 2.0 / ROPE)
    query_pos = ctx * rows + jnp.arange(rows, dtype=jnp.int32)
    angles = query_pos.astype(jnp.float32)[:, None] * frequency[None, :]
    cosine = jnp.cos(angles)
    sine = jnp.sin(angles)
    cos2 = jnp.concatenate([cosine, cosine], axis=1)
    sin2 = jnp.concatenate([-sine, sine], axis=1)
    full_query, start = pl.pallas_call(
        query_kernel,
        out_shape=(jax.ShapeDtypeStruct((heads, rows, WIDTH), bf16),
                   jax.ShapeDtypeStruct((rows, rows), jnp.int32)),
        in_specs=[SMEM] + vmem(5), out_specs=tuple(vmem(2)), name="query",
    )(ctx[None], queries, absorb_key, cos2, sin2, segments.reshape(-1, rows))

    from_head = [(head - k) % head_count for k in range(head_count)]
    meta = jnp.stack(
        [ctx] + [f * dec_count + core for f in from_head]
        + [f * dec_count + (1 - core) for f in from_head]
    )
    group = 2
    state = pl.pallas_call(
        lambda *refs: first_kernel(*refs, scale=scale, group=group),
        out_shape=(jax.ShapeDtypeStruct((heads, rows, 128), jnp.float32),
                   jax.ShapeDtypeStruct((heads, rows, 128), jnp.float32),
                   jax.ShapeDtypeStruct((heads, rows, LATENT), jnp.float32)),
        in_specs=[SMEM] + vmem(5), out_specs=tuple(vmem(3)),
        scratch_shapes=[pltpu.VMEM(((len(EVEN) + 1) * rows, WIDTH), bf16),
                        pltpu.VMEM((rows, (len(EVEN) + 1) * rows), jnp.float32)],
        name="first",
        cost_estimate=pl.CostEstimate(flops=5_000_000_000, bytes_accessed=6_000_000, transcendentals=1_000_000),
    )(meta, full_query, start, latent_rows, near_even, far_even)
    answer = pl.pallas_call(
        lambda *refs: second_kernel(*refs, scale=scale, group=group),
        out_shape=jax.ShapeDtypeStruct((rows, heads * VDIM), bf16),
        in_specs=[SMEM] + vmem(8), out_specs=vmem(1)[0],
        scratch_shapes=[pltpu.VMEM((len(ODD) * rows, WIDTH), bf16),
                        pltpu.VMEM((rows, len(ODD) * rows), jnp.float32)],
        name="second",
        cost_estimate=pl.CostEstimate(flops=5_000_000_000, bytes_accessed=6_000_000, transcendentals=1_000_000),
    )(meta, full_query, start, *state, near_odd, far_odd, absorb_value)
    return (answer, arrived[None])


def solution(mesh):
    in_specs = (
        P(("group", "ctx"), ("head", "dec")),
        P(("group", "ctx"), None),
        P("group"),
        P(("group", "ctx"), None),
        P(("head", "dec"), None, None),
        P(("head", "dec"), None, None),
    )
    out_specs = (P(("group", "ctx"), ("head", "dec")), P(("group", "ctx", "dec"), None, None, None))
    return jax.shard_map(
        on_device, mesh=mesh, in_specs=in_specs, out_specs=out_specs, check_vma=False
    )
```

```python
import jax
import jax.numpy as jnp
from jax import lax
from jax.experimental import pallas as pl
from jax.experimental.pallas import tpu as pltpu
from jax.experimental.layout import Layout, with_layout_constraint
from jax.sharding import PartitionSpec as P


NOPE = 128
ROPE = 64
LATENT = 512
VDIM = 128
WIDTH = LATENT + ROPE
HEAD_IN = NOPE + ROPE
NEG = -1e30
LOG2E = 1.4426950408889634
DISTANCES = (1, 9, 5, 13, 3, 11, 7, 15, 2, 10, 6, 14, 4, 12, 8, 16)


def query_kernel(ctx_ref, q_ref, ak_ref, cos_ref, sin_ref, seg_ref, fq_ref, start_ref):
    heads = ak_ref.shape[0]
    rows = q_ref.shape[0]
    cos2 = cos_ref[...]
    sin2 = sin_ref[...]
    half = ROPE // 2
    for h in range(heads):
        piece = q_ref[:, h * HEAD_IN:(h + 1) * HEAD_IN]
        absorbed = jnp.dot(piece[:, :NOPE], ak_ref[h], preferred_element_type=jnp.float32)
        fq_ref[h, :, :LATENT] = absorbed.astype(jnp.bfloat16)
        x = piece[:, NOPE:].astype(jnp.float32)
        swapped = jnp.concatenate([x[:, half:], x[:, :half]], axis=1)
        fq_ref[h, :, LATENT:] = (x * cos2 + swapped * sin2).astype(jnp.bfloat16)
    own = seg_ref[pl.ds(ctx_ref[0], 1), :]
    own = jnp.broadcast_to(own, (rows, rows)).T
    below = jnp.zeros((rows, rows), jnp.int32)
    for b in range(seg_ref.shape[0]):
        below = below + (seg_ref[b:b + 1, :] < own).astype(jnp.int32)
    start = jnp.sum(below, axis=1, keepdims=True)
    start_ref[...] = jnp.broadcast_to(start, (rows, rows))


def pick_kernel(core_ref, owner_ref, latent_ref, out_ref, *, cores, slots):
    rows = latent_ref.shape[0]
    own = jnp.broadcast_to(owner_ref[...], (rows, rows))
    across = own.T
    down_id = lax.broadcasted_iota(jnp.int32, (rows, rows), 0)
    across_id = lax.broadcasted_iota(jnp.int32, (rows, rows), 1)
    hit = ((own == across) & (down_id < across_id)).astype(jnp.int32)
    rank = jnp.sum(hit, axis=0, keepdims=True)
    name = across[:1, :]
    target = name // cores * slots + rank
    target = jnp.where(name % cores == core_ref[0], target, -1)
    slot_id = lax.broadcasted_iota(jnp.int32, (out_ref.shape[0], rows), 0)
    picker = (slot_id == target).astype(jnp.float32).astype(jnp.bfloat16)
    out_ref[...] = jnp.dot(
        picker, latent_ref[...], preferred_element_type=jnp.float32
    ).astype(jnp.bfloat16)


def attend_kernel(meta_ref, fq_ref, start_ref, latent_ref, near_ref, far_ref, av_ref,
                  out_ref, keys_ref, bias_ref, sems, *, scale, group):
    heads, rows = fq_ref.shape[0], fq_ref.shape[1]
    count = len(DISTANCES)
    quarters = near_ref.shape[0]
    copies = [pltpu.make_async_copy(latent_ref, keys_ref.at[count], sems.at[2 * quarters])]
    for i in range(quarters):
        copies.append(pltpu.make_async_copy(
            near_ref.at[i], keys_ref.at[pl.ds(0, count), meta_ref[1 + i]], sems.at[i]))
        copies.append(pltpu.make_async_copy(
            far_ref.at[i], keys_ref.at[pl.ds(0, count), meta_ref[1 + quarters + i]],
            sems.at[quarters + i]))
    for copy in copies:
        copy.start()
    start = start_ref[...]
    ctx = meta_ref[0]
    lane = lax.broadcasted_iota(jnp.int32, (rows, rows), 1)
    down = lax.broadcasted_iota(jnp.int32, (rows, rows), 0)
    for b, dist in enumerate(DISTANCES):
        seen = (ctx - dist) * rows + lane >= start
        bias_ref[:, b * rows:(b + 1) * rows] = jnp.where(seen, 0.0, NEG)
    seen = (ctx * rows + lane >= start) & (lane <= down)
    bias_ref[:, count * rows:] = jnp.where(seen, 0.0, NEG)
    for copy in copies:
        copy.wait()
    factor = scale * LOG2E
    total_keys = (count + 1) * rows
    for h in range(0, heads, group):
        q = fq_ref[h:h + group].reshape(group * rows, WIDTH)
        keys = keys_ref[...].reshape(total_keys, WIDTH)
        s = lax.dot_general(
            q, keys, (((1,), (1,)), ((), ())), preferred_element_type=jnp.float32
        )
        s = s.reshape(group, rows, total_keys) + bias_ref[...][None]
        top = jnp.max(s, axis=2, keepdims=True)
        p = jnp.exp2((s - top) * factor)
        total = jnp.sum(p, axis=2, keepdims=True)
        mixed = jnp.dot(
            p.astype(jnp.bfloat16).reshape(group * rows, total_keys), keys[:, :LATENT],
            preferred_element_type=jnp.float32,
        ).reshape(group, rows, LATENT)
        mixed = (mixed / total).astype(jnp.bfloat16)
        for g in range(group):
            out_ref[:, (h + g) * VDIM:(h + g + 1) * VDIM] = jnp.dot(
                mixed[g], av_ref[h + g], preferred_element_type=jnp.float32
            ).astype(jnp.bfloat16)


def vmem(n):
    return [pl.BlockSpec(memory_space=pltpu.VMEM) for _ in range(n)]


SMEM = pl.BlockSpec(memory_space=pltpu.SMEM)


def program(queries, latent_rows, segments, owners, absorb_key, absorb_value):
    rows = queries.shape[0]
    heads = absorb_key.shape[0]
    ctx_count = lax.axis_size("ctx")
    head_count = lax.axis_size("head")
    dec_count = lax.axis_size("dec")
    ctx = lax.axis_index("ctx")
    head = lax.axis_index("head")
    core = lax.axis_index("dec")
    scale = (NOPE + ROPE) ** (-0.5)
    bf16 = jnp.bfloat16

    half = ROPE // 2
    frequency = 10000.0 ** (-jnp.arange(half, dtype=jnp.float32) * 2.0 / ROPE)
    query_pos = ctx * rows + jnp.arange(rows, dtype=jnp.int32)
    angles = query_pos.astype(jnp.float32)[:, None] * frequency[None, :]
    cosine = jnp.cos(angles)
    sine = jnp.sin(angles)
    cos2 = jnp.concatenate([cosine, cosine], axis=1)
    sin2 = jnp.concatenate([-sine, sine], axis=1)
    full_query, start = pl.pallas_call(
        query_kernel,
        out_shape=(jax.ShapeDtypeStruct((heads, rows, WIDTH), bf16),
                   jax.ShapeDtypeStruct((rows, rows), jnp.int32)),
        in_specs=[SMEM] + vmem(5), out_specs=tuple(vmem(2)), name="query",
    )(ctx[None], queries, absorb_key, cos2, sin2, segments.reshape(-1, rows))
    from_head = [(head - k) % head_count for k in range(head_count)]
    meta = jnp.stack(
        [ctx] + [f * dec_count + core for f in from_head]
        + [f * dec_count + (1 - core) for f in from_head]
    )

    slots = max(2, 2 * rows // (ctx_count * dec_count))
    outgoing = pl.pallas_call(
        lambda *refs: pick_kernel(*refs, cores=dec_count, slots=slots),
        out_shape=jax.ShapeDtypeStruct((ctx_count * slots, WIDTH), bf16),
        in_specs=[SMEM] + vmem(2), out_specs=vmem(1)[0], name="pick",
    )(core[None], owners, latent_rows)
    outgoing = outgoing.reshape(ctx_count, slots, WIDTH)

    replica = head * dec_count + core
    share = rows // (head_count * dec_count)
    own = lax.dynamic_slice_in_dim(latent_rows, replica * share, share, 0)

    def shift(x, k):
        return lax.ppermute(x, "ctx", [(i, i + k) for i in range(ctx_count - k)])

    def row_major(x):
        return with_layout_constraint(x, Layout((0, 1)))

    def cat(*xs):
        return row_major(jnp.concatenate(xs, axis=0))

    two = cat(shift(own, 1), shift(own, 9))
    two, full_query, start, outgoing, meta = lax.optimization_barrier(
        (two, full_query, start, outgoing, meta))
    four = cat(two, shift(two, 4))
    eight = cat(four, shift(four, 2))
    eight, outgoing = lax.optimization_barrier((eight, outgoing))
    arrived = lax.all_to_all(outgoing, "ctx", split_axis=0, concat_axis=0, tiled=True)
    late = shift(eight, 1)
    window = cat(eight, late)

    ring = lambda k: [(i, (i + k) % head_count) for i in range(head_count)]
    others = [lax.ppermute(window, "head", ring(k)) for k in range(1, head_count)]
    near = cat(window, *others)
    far = row_major(lax.ppermute(near, "dec", [(i, (i + 1) % dec_count) for i in range(dec_count)]))

    blocks = len(DISTANCES)
    parts = head_count * dec_count
    by_share = lambda x: x.reshape(head_count, blocks, share, WIDTH)
    any_spec = pl.BlockSpec(memory_space=pl.ANY)
    answer = pl.pallas_call(
        lambda *refs: attend_kernel(*refs, scale=scale, group=2),
        out_shape=jax.ShapeDtypeStruct((rows, heads * VDIM), bf16),
        in_specs=[SMEM] + vmem(2) + [any_spec] * 3 + vmem(1), out_specs=vmem(1)[0],
        scratch_shapes=[pltpu.VMEM((blocks + 1, parts, share, WIDTH), bf16),
                        pltpu.VMEM((rows, (blocks + 1) * rows), jnp.float32),
                        pltpu.SemaphoreType.DMA((parts + 1,))],
        name="attend",
        cost_estimate=pl.CostEstimate(
            flops=10_000_000_000, bytes_accessed=6_000_000, transcendentals=2_000_000),
    )(meta, full_query, start, latent_rows.reshape(parts, share, WIDTH), by_share(near),
      by_share(far), absorb_value)
    return (answer, arrived[None])


def solution(mesh):
    in_specs = (
        P(("group", "ctx"), ("head", "dec")),
        P(("group", "ctx"), None),
        P("group"),
        P(("group", "ctx"), None),
        P(("head", "dec"), None, None),
        P(("head", "dec"), None, None),
    )
    out_specs = (P(("group", "ctx"), ("head", "dec")), P(("group", "ctx", "dec"), None, None, None))
    return jax.shard_map(
        program, mesh=mesh, in_specs=in_specs, out_specs=out_specs, check_vma=False
    )
```

```python
import jax
import jax.numpy as jnp
from jax import lax
from jax.experimental import pallas as pl
from jax.experimental.pallas import tpu as pltpu
from jax.experimental.layout import Layout, with_layout_constraint
from jax.sharding import PartitionSpec as P


NOPE = 128
ROPE = 64
LATENT = 512
VDIM = 128
WIDTH = LATENT + ROPE
HEAD_IN = NOPE + ROPE
NEG = -1e30
LOG2E = 1.4426950408889634
DISTANCES = (1, 9, 5, 13, 3, 11, 7, 15, 2, 10, 6, 14, 4, 12, 8, 16)


def query_kernel(ctx_ref, q_ref, ak_ref, cos_ref, sin_ref, seg_ref, fq_ref, start_ref):
    heads = ak_ref.shape[0]
    rows = q_ref.shape[0]
    cos2 = cos_ref[...]
    sin2 = sin_ref[...]
    half = ROPE // 2
    for h in range(heads):
        piece = q_ref[:, h * HEAD_IN:(h + 1) * HEAD_IN]
        absorbed = jnp.dot(piece[:, :NOPE], ak_ref[h], preferred_element_type=jnp.float32)
        fq_ref[h, :, :LATENT] = absorbed.astype(jnp.bfloat16)
        x = piece[:, NOPE:].astype(jnp.float32)
        swapped = jnp.concatenate([x[:, half:], x[:, :half]], axis=1)
        fq_ref[h, :, LATENT:] = (x * cos2 + swapped * sin2).astype(jnp.bfloat16)
    own = seg_ref[pl.ds(ctx_ref[0], 1), :]
    own = jnp.broadcast_to(own, (rows, rows)).T
    below = jnp.zeros((rows, rows), jnp.int32)
    for b in range(seg_ref.shape[0]):
        below = below + (seg_ref[b:b + 1, :] < own).astype(jnp.int32)
    start = jnp.sum(below, axis=1, keepdims=True)
    start_ref[...] = jnp.broadcast_to(start, (rows, rows))


def pick_kernel(core_ref, owner_ref, latent_ref, out_ref, *, cores, slots):
    rows = latent_ref.shape[0]
    own = jnp.broadcast_to(owner_ref[...], (rows, rows))
    across = own.T
    down_id = lax.broadcasted_iota(jnp.int32, (rows, rows), 0)
    across_id = lax.broadcasted_iota(jnp.int32, (rows, rows), 1)
    hit = ((own == across) & (down_id < across_id)).astype(jnp.int32)
    rank = jnp.sum(hit, axis=0, keepdims=True)
    name = across[:1, :]
    target = name // cores * slots + rank
    target = jnp.where(name % cores == core_ref[0], target, -1)
    slot_id = lax.broadcasted_iota(jnp.int32, (out_ref.shape[0], rows), 0)
    picker = (slot_id == target).astype(jnp.float32).astype(jnp.bfloat16)
    out_ref[...] = jnp.dot(
        picker, latent_ref[...], preferred_element_type=jnp.float32
    ).astype(jnp.bfloat16)


def attend_kernel(meta_ref, start_ref, fq_hbm, latent_ref, near_ref, far_ref, av_hbm,
                  out_ref, keys_ref, bias_ref, fq_ref, av_ref, sems, *, scale, group):
    heads, rows = fq_ref.shape[0], fq_ref.shape[1]
    count = len(DISTANCES)
    quarters = near_ref.shape[0]
    copies = [pltpu.make_async_copy(latent_ref, keys_ref.at[count], sems.at[2 * quarters])]
    for i in range(quarters):
        copies.append(pltpu.make_async_copy(
            near_ref.at[i], keys_ref.at[pl.ds(0, count), meta_ref[1 + i]], sems.at[i]))
        copies.append(pltpu.make_async_copy(
            far_ref.at[i], keys_ref.at[pl.ds(0, count), meta_ref[1 + quarters + i]],
            sems.at[quarters + i]))
    queries = [
        pltpu.make_async_copy(fq_hbm.at[pl.ds(h, group)], fq_ref.at[pl.ds(h, group)],
                              sems.at[2 * quarters + 1 + h // group])
        for h in range(0, heads, group)
    ]
    values = pltpu.make_async_copy(av_hbm, av_ref, sems.at[2 * quarters + 1 + heads // group])
    for copy in queries[:1] + copies + queries[1:] + [values]:
        copy.start()
    start = start_ref[...]
    ctx = meta_ref[0]
    lane = lax.broadcasted_iota(jnp.int32, (rows, rows), 1)
    down = lax.broadcasted_iota(jnp.int32, (rows, rows), 0)
    for b, dist in enumerate(DISTANCES):
        seen = (ctx - dist) * rows + lane >= start
        bias_ref[:, b * rows:(b + 1) * rows] = jnp.where(seen, 0.0, NEG)
    seen = (ctx * rows + lane >= start) & (lane <= down)
    bias_ref[:, count * rows:] = jnp.where(seen, 0.0, NEG)
    for copy in copies:
        copy.wait()
    factor = scale * LOG2E
    total_keys = (count + 1) * rows
    for h in range(0, heads, group):
        queries[h // group].wait()
        q = fq_ref[h:h + group].reshape(group * rows, WIDTH)
        keys = keys_ref[...].reshape(total_keys, WIDTH)
        s = lax.dot_general(
            q, keys, (((1,), (1,)), ((), ())), preferred_element_type=jnp.float32
        )
        s = s.reshape(group, rows, total_keys) + bias_ref[...][None]
        top = jnp.max(s, axis=2, keepdims=True)
        p = jnp.exp2((s - top) * factor)
        total = jnp.sum(p, axis=2, keepdims=True)
        mixed = jnp.dot(
            p.astype(jnp.bfloat16).reshape(group * rows, total_keys), keys[:, :LATENT],
            preferred_element_type=jnp.float32,
        ).reshape(group, rows, LATENT)
        mixed = (mixed / total).astype(jnp.bfloat16)
        if h == 0:
            values.wait()
        for g in range(group):
            out_ref[:, (h + g) * VDIM:(h + g + 1) * VDIM] = jnp.dot(
                mixed[g], av_ref[h + g], preferred_element_type=jnp.float32
            ).astype(jnp.bfloat16)


def vmem(n):
    return [pl.BlockSpec(memory_space=pltpu.VMEM) for _ in range(n)]


SMEM = pl.BlockSpec(memory_space=pltpu.SMEM)


def program(queries, latent_rows, segments, owners, absorb_key, absorb_value):
    rows = queries.shape[0]
    heads = absorb_key.shape[0]
    ctx_count = lax.axis_size("ctx")
    head_count = lax.axis_size("head")
    dec_count = lax.axis_size("dec")
    ctx = lax.axis_index("ctx")
    head = lax.axis_index("head")
    core = lax.axis_index("dec")
    scale = (NOPE + ROPE) ** (-0.5)
    bf16 = jnp.bfloat16

    half = ROPE // 2
    frequency = 10000.0 ** (-jnp.arange(half, dtype=jnp.float32) * 2.0 / ROPE)
    query_pos = ctx * rows + jnp.arange(rows, dtype=jnp.int32)
    angles = query_pos.astype(jnp.float32)[:, None] * frequency[None, :]
    cosine = jnp.cos(angles)
    sine = jnp.sin(angles)
    cos2 = jnp.concatenate([cosine, cosine], axis=1)
    sin2 = jnp.concatenate([-sine, sine], axis=1)
    full_query, start = pl.pallas_call(
        query_kernel,
        out_shape=(jax.ShapeDtypeStruct((heads, rows, WIDTH), bf16),
                   jax.ShapeDtypeStruct((rows, rows), jnp.int32)),
        in_specs=[SMEM] + vmem(5), out_specs=tuple(vmem(2)), name="query",
    )(ctx[None], queries, absorb_key, cos2, sin2, segments.reshape(-1, rows))
    from_head = [(head - k) % head_count for k in range(head_count)]
    meta = jnp.stack(
        [ctx] + [f * dec_count + core for f in from_head]
        + [f * dec_count + (1 - core) for f in from_head]
    )

    slots = max(2, 2 * rows // (ctx_count * dec_count))
    outgoing = pl.pallas_call(
        lambda *refs: pick_kernel(*refs, cores=dec_count, slots=slots),
        out_shape=jax.ShapeDtypeStruct((ctx_count * slots, WIDTH), bf16),
        in_specs=[SMEM] + vmem(2), out_specs=vmem(1)[0], name="pick",
    )(core[None], owners, latent_rows)
    outgoing = outgoing.reshape(ctx_count, slots, WIDTH)

    replica = head * dec_count + core
    share = rows // (head_count * dec_count)
    own = lax.dynamic_slice_in_dim(latent_rows, replica * share, share, 0)

    def shift(x, k):
        return lax.ppermute(x, "ctx", [(i, i + k) for i in range(ctx_count - k)])

    def row_major(x):
        return with_layout_constraint(x, Layout((0, 1)))

    def cat(*xs):
        return row_major(jnp.concatenate(xs, axis=0))

    ninth = shift(own, 9)
    two = cat(shift(own, 1), ninth)
    four = cat(two, shift(two, 4))
    eight = cat(four, shift(four, 2))
    arrived = lax.all_to_all(outgoing, "ctx", split_axis=0, concat_axis=0, tiled=True)
    late = shift(eight, 1)
    window = cat(eight, late)

    ring = lambda k: [(i, (i + k) % head_count) for i in range(head_count)]
    others = [lax.ppermute(window, "head", ring(k)) for k in range(1, head_count)]
    blocks = len(DISTANCES)
    parts = head_count * dec_count
    group = 2
    near = cat(window, *others).reshape(head_count, blocks, share, WIDTH)
    far = lax.ppermute(near, "dec", [(i, (i + 1) % dec_count) for i in range(dec_count)])
    any_spec = pl.BlockSpec(memory_space=pl.ANY)
    answer = pl.pallas_call(
        lambda *refs: attend_kernel(*refs, scale=scale, group=group),
        out_shape=jax.ShapeDtypeStruct((rows, heads * VDIM), bf16),
        in_specs=[SMEM] + vmem(1) + [any_spec] * 5, out_specs=vmem(1)[0],
        scratch_shapes=[pltpu.VMEM((blocks + 1, parts, share, WIDTH), bf16),
                        pltpu.VMEM((rows, (blocks + 1) * rows), jnp.float32),
                        pltpu.VMEM(full_query.shape, bf16),
                        pltpu.VMEM(absorb_value.shape, bf16),
                        pltpu.SemaphoreType.DMA((parts + 2 + heads // group,))],
        name="attend",
        cost_estimate=pl.CostEstimate(
            flops=10_000_000_000, bytes_accessed=6_000_000, transcendentals=2_000_000),
    )(meta, start, full_query, latent_rows.reshape(parts, share, WIDTH), near, far,
      absorb_value)
    return (answer, arrived[None])


def solution(mesh):
    in_specs = (
        P(("group", "ctx"), ("head", "dec")),
        P(("group", "ctx"), None),
        P("group"),
        P(("group", "ctx"), None),
        P(("head", "dec"), None, None),
        P(("head", "dec"), None, None),
    )
    out_specs = (P(("group", "ctx"), ("head", "dec")), P(("group", "ctx", "dec"), None, None, None))
    return jax.shard_map(
        program, mesh=mesh, in_specs=in_specs, out_specs=out_specs, check_vma=False
    )
```

```python
import jax
import jax.numpy as jnp
import numpy as np
from jax import lax
from jax.experimental import pallas as pl
from jax.experimental.pallas import tpu as pltpu
from jax.experimental.layout import Layout, with_layout_constraint
from jax.sharding import PartitionSpec as P


NOPE = 128
ROPE = 64
LATENT = 512
VDIM = 128
WIDTH = LATENT + ROPE
HEAD_IN = NOPE + ROPE
NEG = -1e30
LOG2E = 1.4426950408889634
EARLY = (1, 9, 5, 13, 3, 11, 7, 15)
LATE = (2, 10, 6, 14, 4, 12, 8, 16)


def query_kernel(ctx_ref, q_ref, ak_ref, cos_ref, sin_ref, seg_ref, fq_ref, start_ref):
    heads = ak_ref.shape[0]
    rows = q_ref.shape[0]
    cos2 = cos_ref[...]
    sin2 = sin_ref[...]
    half = ROPE // 2
    for h in range(heads):
        piece = q_ref[:, h * HEAD_IN:(h + 1) * HEAD_IN]
        absorbed = jnp.dot(piece[:, :NOPE], ak_ref[h], preferred_element_type=jnp.float32)
        fq_ref[h, :, :LATENT] = absorbed.astype(jnp.bfloat16)
        x = piece[:, NOPE:].astype(jnp.float32)
        swapped = jnp.concatenate([x[:, half:], x[:, :half]], axis=1)
        fq_ref[h, :, LATENT:] = (x * cos2 + swapped * sin2).astype(jnp.bfloat16)
    own = seg_ref[pl.ds(ctx_ref[0], 1), :]
    own = jnp.broadcast_to(own, (rows, rows)).T
    below = jnp.zeros((rows, rows), jnp.int32)
    for b in range(seg_ref.shape[0]):
        below = below + (seg_ref[b:b + 1, :] < own).astype(jnp.int32)
    start = jnp.sum(below, axis=1, keepdims=True)
    start_ref[...] = jnp.broadcast_to(start, (rows, rows))


def pick_kernel(core_ref, owner_ref, latent_ref, out_ref, *, cores, slots):
    rows = latent_ref.shape[0]
    own = jnp.broadcast_to(owner_ref[...], (rows, rows))
    across = own.T
    down_id = lax.broadcasted_iota(jnp.int32, (rows, rows), 0)
    across_id = lax.broadcasted_iota(jnp.int32, (rows, rows), 1)
    hit = ((own == across) & (down_id < across_id)).astype(jnp.int32)
    rank = jnp.sum(hit, axis=0, keepdims=True)
    name = across[:1, :]
    target = name // cores * slots + rank
    target = jnp.where(name % cores == core_ref[0], target, -1)
    slot_id = lax.broadcasted_iota(jnp.int32, (out_ref.shape[0], rows), 0)
    picker = (slot_id == target).astype(jnp.float32).astype(jnp.bfloat16)
    out_ref[...] = jnp.dot(
        picker, latent_ref[...], preferred_element_type=jnp.float32
    ).astype(jnp.bfloat16)


def attend_kernel(meta_ref, start_ref, offset_ref, fq_ref, latent_ref, near_early_ref,
                  near_late_ref, far_early_ref, far_late_ref, av_hbm, out_ref, bias_ref, av_ref,
                  sem, *, scale, group):
    heads, rows = fq_ref.shape[0], fq_ref.shape[1]
    parts = (near_early_ref, near_late_ref, far_early_ref, far_late_ref)
    wide = near_early_ref.shape[0]
    pieces = wide // rows
    values = pltpu.make_async_copy(av_hbm, av_ref, sem)
    values.start()
    start = start_ref[...]
    base = meta_ref[0] * rows
    for n in range(len(parts)):
        offset = offset_ref[n % 2:n % 2 + 1, :]
        for i in range(pieces):
            share_start = meta_ref[1 + (n // 2) * pieces + i] * (rows // (2 * pieces))
            seen = base + share_start + offset >= start
            at = n * wide + i * rows
            bias_ref[:, at:at + rows] = jnp.where(seen, 0.0, NEG)
    lane = lax.broadcasted_iota(jnp.int32, (rows, rows), 1)
    down = lax.broadcasted_iota(jnp.int32, (rows, rows), 0)
    bias_ref[:, len(parts) * wide:] = jnp.where(
        (base + lane >= start) & (lane <= down), 0.0, NEG)
    factor = scale * LOG2E
    parts = parts + (latent_ref,)
    for h in range(0, heads, group):
        q = fq_ref[h:h + group].reshape(group * rows, WIDTH)
        scores = []
        for n, part in enumerate(parts):
            s = lax.dot_general(
                q, part[...], (((1,), (1,)), ((), ())), preferred_element_type=jnp.float32
            )
            bias = bias_ref[:, n * wide:n * wide + part.shape[0]]
            scores.append(s.reshape(group, rows, -1) + bias[None])
        s = jnp.concatenate(scores, axis=2)
        top = jnp.max(s, axis=2, keepdims=True)
        p = jnp.exp2((s - top) * factor)
        total = jnp.sum(p, axis=2, keepdims=True)
        p = p.astype(jnp.bfloat16).reshape(group * rows, -1)
        mixed = jnp.zeros((group * rows, LATENT), jnp.float32)
        for n, part in enumerate(parts):
            mixed = mixed + jnp.dot(
                p[:, n * wide:n * wide + part.shape[0]], part[:, :LATENT],
                preferred_element_type=jnp.float32,
            )
        mixed = (mixed.reshape(group, rows, LATENT) / total).astype(jnp.bfloat16)
        if h == 0:
            values.wait()
        for g in range(group):
            out_ref[:, (h + g) * VDIM:(h + g + 1) * VDIM] = jnp.dot(
                mixed[g], av_ref[h + g], preferred_element_type=jnp.float32
            ).astype(jnp.bfloat16)


def vmem(n):
    return [pl.BlockSpec(memory_space=pltpu.VMEM) for _ in range(n)]


def KEEP(x):
    return pltpu.with_memory_space_constraint(x, pltpu.VMEM)


SMEM = pl.BlockSpec(memory_space=pltpu.SMEM)


def program(queries, latent_rows, segments, owners, absorb_key, absorb_value):
    rows = queries.shape[0]
    heads = absorb_key.shape[0]
    ctx_count = lax.axis_size("ctx")
    head_count = lax.axis_size("head")
    dec_count = lax.axis_size("dec")
    ctx = lax.axis_index("ctx")
    head = lax.axis_index("head")
    core = lax.axis_index("dec")
    scale = (NOPE + ROPE) ** (-0.5)
    bf16 = jnp.bfloat16

    half = ROPE // 2
    frequency = 10000.0 ** (-jnp.arange(half, dtype=jnp.float32) * 2.0 / ROPE)
    query_pos = ctx * rows + jnp.arange(rows, dtype=jnp.int32)
    angles = query_pos.astype(jnp.float32)[:, None] * frequency[None, :]
    cosine = jnp.cos(angles)
    sine = jnp.sin(angles)
    cos2 = jnp.concatenate([cosine, cosine], axis=1)
    sin2 = jnp.concatenate([-sine, sine], axis=1)
    full_query, start = pl.pallas_call(
        query_kernel,
        out_shape=(pltpu.VMEM((heads, rows, WIDTH), bf16),
                   pltpu.VMEM((rows, rows), jnp.int32)),
        in_specs=[SMEM] + vmem(5), out_specs=tuple(vmem(2)), name="query", compiler_params=pltpu.CompilerParams(vmem_limit_bytes=16 << 20),
    )(ctx[None], queries, absorb_key, cos2, sin2, segments.reshape(-1, rows))
    from_head = [(head - k) % head_count for k in range(head_count)]
    meta = jnp.stack(
        [ctx] + [f * dec_count + core for f in from_head]
        + [f * dec_count + (1 - core) for f in from_head]
    )

    slots = max(2, 2 * rows // (ctx_count * dec_count))
    outgoing = pl.pallas_call(
        lambda *refs: pick_kernel(*refs, cores=dec_count, slots=slots),
        out_shape=jax.ShapeDtypeStruct((ctx_count * slots, WIDTH), bf16),
        in_specs=[SMEM] + vmem(2), out_specs=vmem(1)[0], name="pick", compiler_params=pltpu.CompilerParams(vmem_limit_bytes=8 << 20),
    )(core[None], owners, latent_rows)
    outgoing = outgoing.reshape(ctx_count, slots, WIDTH)

    replica = head * dec_count + core
    share = rows // (head_count * dec_count)
    own = lax.dynamic_slice_in_dim(latent_rows, replica * share, share, 0)

    def shift(x, k):
        return lax.ppermute(x, "ctx", [(i, i + k) for i in range(ctx_count - k)])

    def row_major(x):
        return with_layout_constraint(x, Layout((0, 1)))

    def cat(*xs):
        return row_major(jnp.concatenate(xs, axis=0))

    ninth = shift(own, 9)
    two = cat(shift(own, 1), ninth)
    four = cat(two, shift(two, 4))
    eight = cat(four, shift(four, 2))
    arrived = lax.all_to_all(outgoing, "ctx", split_axis=0, concat_axis=0, tiled=True)
    late = shift(eight, 1)

    def spread(x):
        others = [
            lax.ppermute(x, "head", [(i, (i + k) % head_count) for i in range(head_count)])
            for k in range(1, head_count)
        ]
        near = cat(x, *others)
        flat = near.reshape(head_count, -1, share, WIDTH)
        far = lax.ppermute(flat, "dec", [(i, (i + 1) % dec_count) for i in range(dec_count)])
        return near, far.reshape(near.shape)

    near_early, far_early = spread(eight)
    near_late, far_late = spread(late)
    offset = jnp.asarray(np.array(
        [[r % share - rows * d[r // share] for r in range(rows)] for d in (EARLY, LATE)], np.int32))
    group = 2
    answer = pl.pallas_call(
        lambda *refs: attend_kernel(*refs, scale=scale, group=group),
        out_shape=jax.ShapeDtypeStruct((rows, heads * VDIM), bf16),
        in_specs=[SMEM] + vmem(8) + [pl.BlockSpec(memory_space=pltpu.HBM)],
        out_specs=vmem(1)[0],
        scratch_shapes=[
            pltpu.VMEM((rows, (1 + len(EARLY) + len(LATE)) * rows), jnp.float32),
            pltpu.VMEM(absorb_value.shape, bf16), pltpu.SemaphoreType.DMA],
        name="attend", compiler_params=pltpu.CompilerParams(vmem_limit_bytes=20 << 20),
        cost_estimate=pl.CostEstimate(
            flops=10_000_000_000, bytes_accessed=6_000_000, transcendentals=2_000_000),
    )(meta, KEEP(start), offset, KEEP(full_query), KEEP(latent_rows), KEEP(near_early),
      KEEP(near_late), KEEP(far_early), KEEP(far_late),
      pltpu.with_memory_space_constraint(absorb_value, pltpu.HBM))
    return (answer, arrived[None])


def solution(mesh):
    in_specs = (
        P(("group", "ctx"), ("head", "dec")),
        P(("group", "ctx"), None),
        P("group"),
        P(("group", "ctx"), None),
        P(("head", "dec"), None, None),
        P(("head", "dec"), None, None),
    )
    out_specs = (P(("group", "ctx"), ("head", "dec")), P(("group", "ctx", "dec"), None, None, None))
    return jax.shard_map(
        program, mesh=mesh, in_specs=in_specs, out_specs=out_specs, check_vma=False
    )
```

```python
import jax
import jax.numpy as jnp
import numpy as np
from jax import lax
from jax.experimental import pallas as pl
from jax.experimental.pallas import tpu as pltpu
from jax.experimental.layout import Layout, with_layout_constraint
from jax.sharding import PartitionSpec as P


NOPE = 128
ROPE = 64
LATENT = 512
VDIM = 128
WIDTH = LATENT + ROPE
HEAD_IN = NOPE + ROPE
NEG = -1e30
LOG2E = 1.4426950408889634
EARLY = (1, 9, 5, 13, 3, 11, 7, 15)
LATE = (2, 10, 6, 14, 4, 12, 8, 16)


def query_kernel(ctx_ref, q_ref, ak_ref, cos_ref, sin_ref, seg_ref, fq_ref, start_ref):
    heads = ak_ref.shape[0]
    rows = q_ref.shape[0]
    cos2 = cos_ref[...]
    sin2 = sin_ref[...]
    half = ROPE // 2
    for h in range(heads):
        piece = q_ref[:, h * HEAD_IN:(h + 1) * HEAD_IN]
        absorbed = jnp.dot(piece[:, :NOPE], ak_ref[h], preferred_element_type=jnp.float32)
        fq_ref[h, :, :LATENT] = absorbed.astype(jnp.bfloat16)
        x = piece[:, NOPE:].astype(jnp.float32)
        swapped = jnp.concatenate([x[:, half:], x[:, :half]], axis=1)
        fq_ref[h, :, LATENT:] = (x * cos2 + swapped * sin2).astype(jnp.bfloat16)
    own = seg_ref[pl.ds(ctx_ref[0], 1), :]
    own = jnp.broadcast_to(own, (rows, rows)).T
    below = jnp.zeros((rows, rows), jnp.int32)
    for b in range(seg_ref.shape[0]):
        below = below + (seg_ref[b:b + 1, :] < own).astype(jnp.int32)
    start = jnp.sum(below, axis=1, keepdims=True)
    start_ref[...] = jnp.broadcast_to(start, (rows, rows))


def pick_kernel(core_ref, owner_ref, latent_ref, out_ref, *, cores, slots):
    rows = latent_ref.shape[0]
    own = jnp.broadcast_to(owner_ref[...], (rows, rows))
    across = own.T
    down_id = lax.broadcasted_iota(jnp.int32, (rows, rows), 0)
    across_id = lax.broadcasted_iota(jnp.int32, (rows, rows), 1)
    hit = ((own == across) & (down_id < across_id)).astype(jnp.int32)
    rank = jnp.sum(hit, axis=0, keepdims=True)
    name = across[:1, :]
    target = name // cores * slots + rank
    target = jnp.where(name % cores == core_ref[0], target, -1)
    slot_id = lax.broadcasted_iota(jnp.int32, (out_ref.shape[0], rows), 0)
    picker = (slot_id == target).astype(jnp.float32).astype(jnp.bfloat16)
    out_ref[...] = jnp.dot(
        picker, latent_ref[...], preferred_element_type=jnp.float32
    ).astype(jnp.bfloat16)


def attend_kernel(meta_ref, start_ref, offset_ref, fq_ref, latent_ref, near_ref, far_ref,
                  av_hbm, out_ref, bias_ref, av_ref, sem, *, scale, group):
    heads, rows = fq_ref.shape[0], fq_ref.shape[1]
    parts = (near_ref, far_ref)
    wide = near_ref.shape[0]
    pieces = wide // (2 * rows)
    values = pltpu.make_async_copy(av_hbm, av_ref, sem)
    values.start()
    start = start_ref[...]
    base = meta_ref[0] * rows
    for n in range(len(parts)):
        for i in range(pieces):
            share_start = meta_ref[1 + n * pieces + i] * (rows // (2 * pieces))
            for k in range(2):
                seen = base + share_start + offset_ref[k:k + 1, :] >= start
                at = n * wide + (2 * i + k) * rows
                bias_ref[:, at:at + rows] = jnp.where(seen, 0.0, NEG)
    lane = lax.broadcasted_iota(jnp.int32, (rows, rows), 1)
    down = lax.broadcasted_iota(jnp.int32, (rows, rows), 0)
    bias_ref[:, len(parts) * wide:] = jnp.where(
        (base + lane >= start) & (lane <= down), 0.0, NEG)
    factor = scale * LOG2E
    parts = parts + (latent_ref,)
    for h in range(0, heads, group):
        q = fq_ref[h:h + group].reshape(group * rows, WIDTH)
        scores = []
        for n, part in enumerate(parts):
            s = lax.dot_general(
                q, part[...], (((1,), (1,)), ((), ())), preferred_element_type=jnp.float32
            )
            bias = bias_ref[:, n * wide:n * wide + part.shape[0]]
            scores.append(s.reshape(group, rows, -1) + bias[None])
        s = jnp.concatenate(scores, axis=2)
        top = jnp.max(s, axis=2, keepdims=True)
        p = jnp.exp2((s - top) * factor)
        total = jnp.sum(p, axis=2, keepdims=True)
        p = p.astype(jnp.bfloat16).reshape(group * rows, -1)
        mixed = jnp.zeros((group * rows, LATENT), jnp.float32)
        for n, part in enumerate(parts):
            mixed = mixed + jnp.dot(
                p[:, n * wide:n * wide + part.shape[0]], part[:, :LATENT],
                preferred_element_type=jnp.float32,
            )
        mixed = (mixed.reshape(group, rows, LATENT) / total).astype(jnp.bfloat16)
        if h == 0:
            values.wait()
        for g in range(group):
            out_ref[:, (h + g) * VDIM:(h + g + 1) * VDIM] = jnp.dot(
                mixed[g], av_ref[h + g], preferred_element_type=jnp.float32
            ).astype(jnp.bfloat16)


def vmem(n):
    return [pl.BlockSpec(memory_space=pltpu.VMEM) for _ in range(n)]


def KEEP(x):
    return pltpu.with_memory_space_constraint(x, pltpu.VMEM)


SMEM = pl.BlockSpec(memory_space=pltpu.SMEM)


def program(queries, latent_rows, segments, owners, absorb_key, absorb_value):
    rows = queries.shape[0]
    heads = absorb_key.shape[0]
    ctx_count = lax.axis_size("ctx")
    head_count = lax.axis_size("head")
    dec_count = lax.axis_size("dec")
    ctx = lax.axis_index("ctx")
    head = lax.axis_index("head")
    core = lax.axis_index("dec")
    scale = (NOPE + ROPE) ** (-0.5)
    bf16 = jnp.bfloat16

    half = ROPE // 2
    frequency = 10000.0 ** (-jnp.arange(half, dtype=jnp.float32) * 2.0 / ROPE)
    query_pos = ctx * rows + jnp.arange(rows, dtype=jnp.int32)
    angles = query_pos.astype(jnp.float32)[:, None] * frequency[None, :]
    cosine = jnp.cos(angles)
    sine = jnp.sin(angles)
    cos2 = jnp.concatenate([cosine, cosine], axis=1)
    sin2 = jnp.concatenate([-sine, sine], axis=1)
    full_query, start = pl.pallas_call(
        query_kernel,
        out_shape=(pltpu.VMEM((heads, rows, WIDTH), bf16),
                   pltpu.VMEM((rows, rows), jnp.int32)),
        in_specs=[SMEM] + vmem(5), out_specs=tuple(vmem(2)), name="query", compiler_params=pltpu.CompilerParams(vmem_limit_bytes=16 << 20),
    )(ctx[None], queries, absorb_key, cos2, sin2, segments.reshape(-1, rows))
    from_head = [(head - k) % head_count for k in range(head_count)]
    meta = jnp.stack(
        [ctx] + [f * dec_count + core for f in from_head]
        + [f * dec_count + (1 - core) for f in from_head]
    )

    slots = max(2, 2 * rows // (ctx_count * dec_count))
    outgoing = pl.pallas_call(
        lambda *refs: pick_kernel(*refs, cores=dec_count, slots=slots),
        out_shape=jax.ShapeDtypeStruct((ctx_count * slots, WIDTH), bf16),
        in_specs=[SMEM] + vmem(2), out_specs=vmem(1)[0], name="pick", compiler_params=pltpu.CompilerParams(vmem_limit_bytes=8 << 20),
    )(core[None], owners, latent_rows)
    outgoing = outgoing.reshape(ctx_count, slots, WIDTH)

    replica = head * dec_count + core
    share = rows // (head_count * dec_count)
    own = lax.dynamic_slice_in_dim(latent_rows, replica * share, share, 0)

    def shift(x, k):
        return lax.ppermute(x, "ctx", [(i, i + k) for i in range(ctx_count - k)])

    def row_major(x):
        return with_layout_constraint(x, Layout((0, 1)))

    def cat(*xs):
        return row_major(jnp.concatenate(xs, axis=0))

    ninth = shift(own, 9)
    two = cat(shift(own, 1), ninth)
    four = cat(two, shift(two, 4))
    eight = cat(four, shift(four, 2))
    arrived = lax.all_to_all(outgoing, "ctx", split_axis=0, concat_axis=0, tiled=True)
    late = shift(eight, 1)

    window = cat(eight, late)
    others = [
        lax.ppermute(window, "head", [(i, (i + k) % head_count) for i in range(head_count)])
        for k in range(1, head_count)
    ]
    near = cat(window, *others)
    near = near.reshape(head_count, 2 * len(EARLY), share, WIDTH)
    far = lax.ppermute(near, "dec", [(i, (i + 1) % dec_count) for i in range(dec_count)])
    keys = lambda x: KEEP(x.reshape(head_count * 2 * rows, WIDTH))
    offset = jnp.asarray(np.array(
        [[r % share - rows * d[r // share] for r in range(rows)] for d in (EARLY, LATE)], np.int32))
    group = 2
    answer = pl.pallas_call(
        lambda *refs: attend_kernel(*refs, scale=scale, group=group),
        out_shape=jax.ShapeDtypeStruct((rows, heads * VDIM), bf16),
        in_specs=[SMEM] + vmem(6) + [pl.BlockSpec(memory_space=pltpu.HBM)],
        out_specs=vmem(1)[0],
        scratch_shapes=[
            pltpu.VMEM((rows, (1 + len(EARLY) + len(LATE)) * rows), jnp.float32),
            pltpu.VMEM(absorb_value.shape, bf16), pltpu.SemaphoreType.DMA],
        name="attend", compiler_params=pltpu.CompilerParams(vmem_limit_bytes=20 << 20),
        cost_estimate=pl.CostEstimate(
            flops=10_000_000_000, bytes_accessed=6_000_000, transcendentals=2_000_000),
    )(meta, KEEP(start), offset, KEEP(full_query), KEEP(latent_rows), keys(near), keys(far),
      pltpu.with_memory_space_constraint(absorb_value, pltpu.HBM))
    return (answer, arrived[None])


def solution(mesh):
    in_specs = (
        P(("group", "ctx"), ("head", "dec")),
        P(("group", "ctx"), None),
        P("group"),
        P(("group", "ctx"), None),
        P(("head", "dec"), None, None),
        P(("head", "dec"), None, None),
    )
    out_specs = (P(("group", "ctx"), ("head", "dec")), P(("group", "ctx", "dec"), None, None, None))
    return jax.shard_map(
        program, mesh=mesh, in_specs=in_specs, out_specs=out_specs, check_vma=False
    )
```

```python
import jax
import jax.numpy as jnp
import numpy as np
from jax import lax
from jax.experimental import pallas as pl
from jax.experimental.pallas import tpu as pltpu
from jax.experimental.layout import Layout, with_layout_constraint
from jax.sharding import PartitionSpec as P


NOPE = 128
ROPE = 64
LATENT = 512
VDIM = 128
WIDTH = LATENT + ROPE
HEAD_IN = NOPE + ROPE
NEG = -1e30
LOG2E = 1.4426950408889634
EARLY = (1, 9, 5, 13, 3, 11, 7, 15)
LATE = (2, 10, 6, 14, 4, 12, 8, 16)


def query_kernel(ctx_ref, q_ref, ak_ref, cos_ref, sin_ref, seg_ref, fq_ref, start_ref):
    heads = ak_ref.shape[0]
    rows = q_ref.shape[0]
    cos2 = cos_ref[...]
    sin2 = sin_ref[...]
    half = ROPE // 2
    for h in range(heads):
        piece = q_ref[:, h * HEAD_IN:(h + 1) * HEAD_IN]
        absorbed = jnp.dot(piece[:, :NOPE], ak_ref[h], preferred_element_type=jnp.float32)
        fq_ref[h, :, :LATENT] = absorbed.astype(jnp.bfloat16)
        x = piece[:, NOPE:].astype(jnp.float32)
        swapped = jnp.concatenate([x[:, half:], x[:, :half]], axis=1)
        fq_ref[h, :, LATENT:] = (x * cos2 + swapped * sin2).astype(jnp.bfloat16)
    own = seg_ref[pl.ds(ctx_ref[0], 1), :]
    own = jnp.broadcast_to(own, (rows, rows)).T
    below = jnp.zeros((rows, rows), jnp.int32)
    for b in range(seg_ref.shape[0]):
        below = below + (seg_ref[b:b + 1, :] < own).astype(jnp.int32)
    start = jnp.sum(below, axis=1, keepdims=True)
    start_ref[...] = jnp.broadcast_to(start, (rows, rows))


def pick_kernel(core_ref, owner_ref, latent_ref, out_ref, *, cores, slots):
    rows = latent_ref.shape[0]
    own = jnp.broadcast_to(owner_ref[...], (rows, rows))
    across = own.T
    down_id = lax.broadcasted_iota(jnp.int32, (rows, rows), 0)
    across_id = lax.broadcasted_iota(jnp.int32, (rows, rows), 1)
    hit = ((own == across) & (down_id < across_id)).astype(jnp.int32)
    rank = jnp.sum(hit, axis=0, keepdims=True)
    name = across[:1, :]
    target = name // cores * slots + rank
    target = jnp.where(name % cores == core_ref[0], target, -1)
    slot_id = lax.broadcasted_iota(jnp.int32, (out_ref.shape[0], rows), 0)
    picker = (slot_id == target).astype(jnp.float32).astype(jnp.bfloat16)
    out_ref[...] = jnp.dot(
        picker, latent_ref[...], preferred_element_type=jnp.float32
    ).astype(jnp.bfloat16)


def attend_kernel(meta_ref, start_ref, offset_ref, fq_ref, *refs, scale, group, shares, skip, own, last):
    heads, rows = fq_ref.shape[0], fq_ref.shape[1]
    refs = list(refs)
    keys_ref = refs.pop(0)
    parts = [keys_ref.at[pl.ds(skip, keys_ref.shape[0] - skip)]]
    if own:
        parts.append(refs.pop(0))
    else:
        max_ref, sum_ref, acc_ref = refs.pop(0), refs.pop(0), refs.pop(0)
    if last:
        av_hbm, out_ref, bias_ref, av_ref, sem = refs
        values = pltpu.make_async_copy(av_hbm, av_ref, sem)
        values.start()
    else:
        new_max_ref, new_sum_ref, new_acc_ref, bias_ref = refs
    start = start_ref[...]
    base = meta_ref[0] * rows
    for i, slot in enumerate(shares):
        share_start = meta_ref[slot]
        for k in range(2):
            seen = base + share_start + offset_ref[k:k + 1, :] >= start
            at = (2 * i + k) * rows
            bias_ref[:, at:at + rows] = jnp.where(seen, 0.0, NEG)
    wide = parts[0].shape[0]
    if own:
        lane = lax.broadcasted_iota(jnp.int32, (rows, rows), 1)
        down = lax.broadcasted_iota(jnp.int32, (rows, rows), 0)
        bias_ref[:, wide:] = jnp.where((base + lane >= start) & (lane <= down), 0.0, NEG)
    factor = scale * LOG2E
    for h in range(0, heads, group):
        q = fq_ref[h:h + group].reshape(group * rows, WIDTH)
        scores = []
        for n, part in enumerate(parts):
            s = lax.dot_general(
                q, part[...], (((1,), (1,)), ((), ())), preferred_element_type=jnp.float32
            )
            bias = bias_ref[:, n * wide:n * wide + part.shape[0]]
            scores.append(s.reshape(group, rows, -1) + bias[None])
        s = jnp.concatenate(scores, axis=2)
        top = jnp.max(s, axis=2, keepdims=True)
        if not own:
            before = max_ref[h:h + group][:, :, :1]
            top = jnp.maximum(before, top)
        p = jnp.exp2((s - top) * factor)
        total = jnp.sum(p, axis=2, keepdims=True)
        p = p.astype(jnp.bfloat16).reshape(group * rows, -1)
        mixed = jnp.dot(p[:, :wide], parts[0][:, :LATENT], preferred_element_type=jnp.float32)
        if own:
            mixed = mixed + jnp.dot(
                p[:, wide:], parts[1][:, :LATENT], preferred_element_type=jnp.float32)
        mixed = mixed.reshape(group, rows, LATENT)
        if not own:
            keep = jnp.exp2((before - top) * factor)
            total = total + sum_ref[h:h + group][:, :, :1] * keep
            mixed = mixed + acc_ref[h:h + group] * keep
        if not last:
            new_max_ref[h:h + group] = jnp.broadcast_to(top, (group, rows, 128))
            new_sum_ref[h:h + group] = jnp.broadcast_to(total, (group, rows, 128))
            new_acc_ref[h:h + group] = mixed
            continue
        mixed = (mixed / total).astype(jnp.bfloat16)
        if h == 0:
            values.wait()
        for g in range(group):
            out_ref[:, (h + g) * VDIM:(h + g + 1) * VDIM] = jnp.dot(
                mixed[g], av_ref[h + g], preferred_element_type=jnp.float32
            ).astype(jnp.bfloat16)


def vmem(n):
    return [pl.BlockSpec(memory_space=pltpu.VMEM) for _ in range(n)]


def KEEP(x):
    return pltpu.with_memory_space_constraint(x, pltpu.VMEM)


SMEM = pl.BlockSpec(memory_space=pltpu.SMEM)


def program(queries, latent_rows, segments, owners, absorb_key, absorb_value):
    rows = queries.shape[0]
    heads = absorb_key.shape[0]
    ctx_count = lax.axis_size("ctx")
    head_count = lax.axis_size("head")
    dec_count = lax.axis_size("dec")
    ctx = lax.axis_index("ctx")
    head = lax.axis_index("head")
    core = lax.axis_index("dec")
    scale = (NOPE + ROPE) ** (-0.5)
    bf16 = jnp.bfloat16

    half = ROPE // 2
    frequency = 10000.0 ** (-jnp.arange(half, dtype=jnp.float32) * 2.0 / ROPE)
    query_pos = ctx * rows + jnp.arange(rows, dtype=jnp.int32)
    angles = query_pos.astype(jnp.float32)[:, None] * frequency[None, :]
    cosine = jnp.cos(angles)
    sine = jnp.sin(angles)
    cos2 = jnp.concatenate([cosine, cosine], axis=1)
    sin2 = jnp.concatenate([-sine, sine], axis=1)
    full_query, start = pl.pallas_call(
        query_kernel,
        out_shape=(pltpu.VMEM((heads, rows, WIDTH), bf16),
                   pltpu.VMEM((rows, rows), jnp.int32)),
        in_specs=[SMEM] + vmem(5), out_specs=tuple(vmem(2)), name="query", compiler_params=pltpu.CompilerParams(vmem_limit_bytes=16 << 20),
    )(ctx[None], queries, absorb_key, cos2, sin2, segments.reshape(-1, rows))
    share = rows // (head_count * dec_count)
    from_head = [(head - k) % head_count for k in range(head_count)]
    meta = jnp.stack(
        [ctx] + [(f * dec_count + core) * share for f in from_head]
        + [(f * dec_count + 1 - core) * share for f in from_head]
    )

    slots = max(2, 2 * rows // (ctx_count * dec_count))
    outgoing = pl.pallas_call(
        lambda *refs: pick_kernel(*refs, cores=dec_count, slots=slots),
        out_shape=jax.ShapeDtypeStruct((ctx_count * slots, WIDTH), bf16),
        in_specs=[SMEM] + vmem(2), out_specs=vmem(1)[0], name="pick", compiler_params=pltpu.CompilerParams(vmem_limit_bytes=8 << 20),
    )(core[None], owners, latent_rows)
    outgoing = outgoing.reshape(ctx_count, slots, WIDTH)

    replica = head * dec_count + core
    share = rows // (head_count * dec_count)
    own = lax.dynamic_slice_in_dim(latent_rows, replica * share, share, 0)

    def shift(x, k):
        return lax.ppermute(x, "ctx", [(i, i + k) for i in range(ctx_count - k)])

    def row_major(x):
        return with_layout_constraint(x, Layout((0, 1)))

    def cat(*xs):
        return row_major(jnp.concatenate(xs, axis=0))

    ninth = shift(own, 9)
    two = cat(shift(own, 1), ninth)
    four = cat(two, shift(two, 4))
    eight = cat(four, shift(four, 2))
    arrived = lax.all_to_all(outgoing, "ctx", split_axis=0, concat_axis=0, tiled=True)
    late = shift(eight, 1)

    window = cat(eight, late)
    others = [
        lax.ppermute(window, "head", [(i, (i + k) % head_count) for i in range(head_count)])
        for k in range(1, head_count)
    ]
    near_flat = cat(window, *others)
    near = near_flat.reshape(head_count, 2 * len(EARLY), share, WIDTH)
    far = lax.ppermute(near, "dec", [(i, (i + 1) % dec_count) for i in range(dec_count)])
    offset = jnp.asarray(np.array(
        [[r % share - rows * d[r // share] for r in range(rows)] for d in (EARLY, LATE)], np.int32))
    group = 2
    state_shape = (pltpu.VMEM((heads, rows, 128), jnp.float32),
                   pltpu.VMEM((heads, rows, 128), jnp.float32),
                   pltpu.VMEM((heads, rows, LATENT), jnp.float32))

    def attend(keys, shares, skip=0, state=(), own=(), values=()):
        count = keys.shape[0] - skip + sum(x.shape[0] for x in own)
        inputs = [KEEP(start), offset, KEEP(full_query), KEEP(keys)]
        inputs += [KEEP(x) for x in own] + [KEEP(x) for x in state]
        scratch = [pltpu.VMEM((rows, count), jnp.float32)]
        if values:
            scratch += [pltpu.VMEM(values[0].shape, bf16), pltpu.SemaphoreType.DMA]
        specs = [SMEM] + vmem(len(inputs)) + [pl.BlockSpec(memory_space=pltpu.HBM) for _ in values]
        inputs += [pltpu.with_memory_space_constraint(x, pltpu.HBM) for x in values]
        out = jax.ShapeDtypeStruct((rows, heads * VDIM), bf16)
        return pl.pallas_call(
            lambda *refs: attend_kernel(*refs, scale=scale, group=group, shares=shares,
                                        skip=skip, own=bool(own), last=bool(values)),
            out_shape=out if values else state_shape,
            in_specs=specs, out_specs=vmem(1)[0] if values else tuple(vmem(3)),
            scratch_shapes=scratch,
            compiler_params=pltpu.CompilerParams(vmem_limit_bytes=20 << 20),
            cost_estimate=pl.CostEstimate(
                flops=2_300_000 * count, bytes_accessed=6_000_000,
                transcendentals=1000 * count),
        )(meta, *inputs)

    state = attend(window, (1,), own=(latent_rows,))
    wide = window.shape[0]
    state = attend(near_flat, (2, 3, 4), skip=wide, state=state)
    answer = attend(far.reshape(near_flat.shape), (5, 6, 7, 8), state=state,
                    values=(absorb_value,))
    return (answer, arrived[None])


def solution(mesh):
    in_specs = (
        P(("group", "ctx"), ("head", "dec")),
        P(("group", "ctx"), None),
        P("group"),
        P(("group", "ctx"), None),
        P(("head", "dec"), None, None),
        P(("head", "dec"), None, None),
    )
    out_specs = (P(("group", "ctx"), ("head", "dec")), P(("group", "ctx", "dec"), None, None, None))
    return jax.shard_map(program, mesh=mesh, in_specs=in_specs, out_specs=out_specs, check_vma=False)
```

```python
import jax
import jax.numpy as jnp
import numpy as np
from jax import lax
from jax.experimental import pallas as pl
from jax.experimental.pallas import tpu as pltpu
from jax.experimental.layout import Layout, with_layout_constraint
from jax.sharding import PartitionSpec as P


NOPE = 128
ROPE = 64
LATENT = 512
VDIM = 128
WIDTH = LATENT + ROPE
HEAD_IN = NOPE + ROPE
NEG = -1e30
LOG2E = 1.4426950408889634
EARLY = (1, 9, 5, 13, 3, 11, 7, 15)
LATE = (2, 10, 6, 14, 4, 12, 8, 16)


def query_kernel(ctx_ref, q_ref, ak_ref, cos_ref, sin_ref, seg_ref, fq_ref, start_ref):
    heads = ak_ref.shape[0]
    rows = q_ref.shape[0]
    cos2 = cos_ref[...]
    sin2 = sin_ref[...]
    half = ROPE // 2
    for h in range(heads):
        piece = q_ref[:, h * HEAD_IN:(h + 1) * HEAD_IN]
        absorbed = jnp.dot(piece[:, :NOPE], ak_ref[h], preferred_element_type=jnp.float32)
        fq_ref[h, :, :LATENT] = absorbed.astype(jnp.bfloat16)
        x = piece[:, NOPE:].astype(jnp.float32)
        swapped = jnp.concatenate([x[:, half:], x[:, :half]], axis=1)
        fq_ref[h, :, LATENT:] = (x * cos2 + swapped * sin2).astype(jnp.bfloat16)
    own = seg_ref[pl.ds(ctx_ref[0], 1), :]
    own = jnp.broadcast_to(own, (rows, rows)).T
    below = jnp.zeros((rows, rows), jnp.int32)
    for b in range(seg_ref.shape[0]):
        below = below + (seg_ref[b:b + 1, :] < own).astype(jnp.int32)
    start = jnp.sum(below, axis=1, keepdims=True)
    start_ref[...] = jnp.broadcast_to(start, (rows, rows))


def pick_kernel(core_ref, owner_ref, latent_ref, out_ref, *, cores, slots):
    rows = latent_ref.shape[0]
    own = jnp.broadcast_to(owner_ref[...], (rows, rows))
    across = own.T
    down_id = lax.broadcasted_iota(jnp.int32, (rows, rows), 0)
    across_id = lax.broadcasted_iota(jnp.int32, (rows, rows), 1)
    hit = ((own == across) & (down_id < across_id)).astype(jnp.int32)
    rank = jnp.sum(hit, axis=0, keepdims=True)
    name = across[:1, :]
    target = name // cores * slots + rank
    target = jnp.where(name % cores == core_ref[0], target, -1)
    slot_id = lax.broadcasted_iota(jnp.int32, (out_ref.shape[0], rows), 0)
    picker = (slot_id == target).astype(jnp.float32).astype(jnp.bfloat16)
    out_ref[...] = jnp.dot(
        picker, latent_ref[...], preferred_element_type=jnp.float32
    ).astype(jnp.bfloat16)


def attend_kernel(meta_ref, start_ref, offset_ref, fq_ref, *refs, scale, group, shares, skip, own, last):
    heads, rows = fq_ref.shape[0], fq_ref.shape[1]
    refs = list(refs)
    keys_ref = refs.pop(0)
    parts = [keys_ref.at[pl.ds(skip, keys_ref.shape[0] - skip)]]
    if own:
        parts.append(refs.pop(0))
    else:
        max_ref, sum_ref, acc_ref = refs.pop(0), refs.pop(0), refs.pop(0)
    if last:
        av_hbm, out_ref, bias_ref, av_ref, sem = refs
        values = pltpu.make_async_copy(av_hbm, av_ref, sem)
        values.start()
    else:
        new_max_ref, new_sum_ref, new_acc_ref, bias_ref = refs
    start = start_ref[...]
    base = meta_ref[0] * rows
    for i, slot in enumerate(shares):
        share_start = meta_ref[slot]
        for k in range(2):
            seen = base + share_start + offset_ref[k:k + 1, :] >= start
            at = (2 * i + k) * rows
            bias_ref[:, at:at + rows] = jnp.where(seen, 0.0, NEG)
    wide = parts[0].shape[0]
    if own:
        lane = lax.broadcasted_iota(jnp.int32, (rows, rows), 1)
        down = lax.broadcasted_iota(jnp.int32, (rows, rows), 0)
        bias_ref[:, wide:] = jnp.where((base + lane >= start) & (lane <= down), 0.0, NEG)
    factor = scale * LOG2E
    for h in range(0, heads, group):
        q = fq_ref[h:h + group].reshape(group * rows, WIDTH)
        scores = []
        for n, part in enumerate(parts):
            s = lax.dot_general(
                q, part[...], (((1,), (1,)), ((), ())), preferred_element_type=jnp.float32
            )
            bias = bias_ref[:, n * wide:n * wide + part.shape[0]]
            scores.append(s.reshape(group, rows, -1) + bias[None])
        s = jnp.concatenate(scores, axis=2)
        top = jnp.max(s, axis=2, keepdims=True)
        if not own:
            before = max_ref[h:h + group][:, :, :1]
            top = jnp.maximum(before, top)
        p = jnp.exp2((s - top) * factor)
        total = jnp.sum(p, axis=2, keepdims=True)
        p = p.astype(jnp.bfloat16).reshape(group * rows, -1)
        mixed = jnp.dot(p[:, :wide], parts[0][:, :LATENT], preferred_element_type=jnp.float32)
        if own:
            mixed = mixed + jnp.dot(
                p[:, wide:], parts[1][:, :LATENT], preferred_element_type=jnp.float32)
        mixed = mixed.reshape(group, rows, LATENT)
        if not own:
            keep = jnp.exp2((before - top) * factor)
            total = total + sum_ref[h:h + group][:, :, :1] * keep
            mixed = mixed + acc_ref[h:h + group] * keep
        if not last:
            new_max_ref[h:h + group] = jnp.broadcast_to(top, (group, rows, 128))
            new_sum_ref[h:h + group] = jnp.broadcast_to(total, (group, rows, 128))
            new_acc_ref[h:h + group] = mixed
            continue
        mixed = (mixed / total).astype(jnp.bfloat16)
        if h == 0:
            values.wait()
        for g in range(group):
            out_ref[:, (h + g) * VDIM:(h + g + 1) * VDIM] = jnp.dot(
                mixed[g], av_ref[h + g], preferred_element_type=jnp.float32
            ).astype(jnp.bfloat16)


def vmem(n):
    return [pl.BlockSpec(memory_space=pltpu.VMEM) for _ in range(n)]


def KEEP(x):
    return pltpu.with_memory_space_constraint(x, pltpu.VMEM)


SMEM = pl.BlockSpec(memory_space=pltpu.SMEM)


def program(queries, latent_rows, segments, owners, absorb_key, absorb_value):
    rows = queries.shape[0]
    heads = absorb_key.shape[0]
    ctx_count = lax.axis_size("ctx")
    head_count = lax.axis_size("head")
    dec_count = lax.axis_size("dec")
    ctx = lax.axis_index("ctx")
    head = lax.axis_index("head")
    core = lax.axis_index("dec")
    scale = (NOPE + ROPE) ** (-0.5)
    bf16 = jnp.bfloat16

    half = ROPE // 2
    frequency = 10000.0 ** (-jnp.arange(half, dtype=jnp.float32) * 2.0 / ROPE)
    query_pos = ctx * rows + jnp.arange(rows, dtype=jnp.int32)
    angles = query_pos.astype(jnp.float32)[:, None] * frequency[None, :]
    cosine = jnp.cos(angles)
    sine = jnp.sin(angles)
    cos2 = jnp.concatenate([cosine, cosine], axis=1)
    sin2 = jnp.concatenate([-sine, sine], axis=1)
    full_query, start = pl.pallas_call(
        query_kernel,
        out_shape=(pltpu.VMEM((heads, rows, WIDTH), bf16),
                   pltpu.VMEM((rows, rows), jnp.int32)),
        in_specs=[SMEM] + vmem(5), out_specs=tuple(vmem(2)), name="query", compiler_params=pltpu.CompilerParams(vmem_limit_bytes=16 << 20),
    )(ctx[None], queries, absorb_key, cos2, sin2, segments.reshape(-1, rows))
    share = rows // (head_count * dec_count)
    from_head = [(head - k) % head_count for k in range(head_count)]
    meta = jnp.stack(
        [ctx] + [(f * dec_count + core) * share for f in from_head]
        + [(f * dec_count + 1 - core) * share for f in from_head]
    )

    slots = max(2, 2 * rows // (ctx_count * dec_count))
    outgoing = pl.pallas_call(
        lambda *refs: pick_kernel(*refs, cores=dec_count, slots=slots),
        out_shape=jax.ShapeDtypeStruct((ctx_count * slots, WIDTH), bf16),
        in_specs=[SMEM] + vmem(2), out_specs=vmem(1)[0], name="pick", compiler_params=pltpu.CompilerParams(vmem_limit_bytes=8 << 20),
    )(core[None], owners, latent_rows)
    outgoing = outgoing.reshape(ctx_count, slots, WIDTH)

    replica = head * dec_count + core
    share = rows // (head_count * dec_count)
    own = lax.dynamic_slice_in_dim(latent_rows, replica * share, share, 0)

    def shift(x, k):
        return lax.ppermute(x, "ctx", [(i, i + k) for i in range(ctx_count - k)])

    def row_major(x):
        return with_layout_constraint(x, Layout((0, 1)))

    def cat(*xs):
        return row_major(jnp.concatenate(xs, axis=0))

    ninth = shift(own, 9)
    two = cat(shift(own, 1), ninth)
    four = cat(two, shift(two, 4))
    eight = cat(four, shift(four, 2))
    arrived = lax.all_to_all(outgoing, "ctx", split_axis=0, concat_axis=0, tiled=True)
    late = shift(eight, 1)

    window = cat(eight, late)

    def turn(k):
        return lax.ppermute(window, "head", [(i, (i + k) % head_count) for i in range(head_count)])

    others = [turn(1)]
    others += [turn(k) for k in range(2, head_count)]
    near_flat = cat(window, *others)
    near = near_flat.reshape(head_count, 2 * len(EARLY), share, WIDTH)
    far = lax.ppermute(near, "dec", [(i, (i + 1) % dec_count) for i in range(dec_count)])
    offset = jnp.asarray(np.array(
        [[r % share - rows * d[r // share] for r in range(rows)] for d in (EARLY, LATE)], np.int32))
    group = 2
    state_shape = (pltpu.VMEM((heads, rows, 128), jnp.float32),
                   pltpu.VMEM((heads, rows, 128), jnp.float32),
                   pltpu.VMEM((heads, rows, LATENT), jnp.float32))

    def attend(keys, shares, skip=0, state=(), own=(), values=()):
        count = keys.shape[0] - skip + sum(x.shape[0] for x in own)
        inputs = [KEEP(start), offset, KEEP(full_query), KEEP(keys)]
        inputs += [KEEP(x) for x in own] + [KEEP(x) for x in state]
        scratch = [pltpu.VMEM((rows, count), jnp.float32)]
        if values:
            scratch += [pltpu.VMEM(values[0].shape, bf16), pltpu.SemaphoreType.DMA]
        specs = [SMEM] + vmem(len(inputs)) + [pl.BlockSpec(memory_space=pltpu.HBM) for _ in values]
        inputs += [pltpu.with_memory_space_constraint(x, pltpu.HBM) for x in values]
        out = jax.ShapeDtypeStruct((rows, heads * VDIM), bf16)
        return pl.pallas_call(
            lambda *refs: attend_kernel(*refs, scale=scale, group=group, shares=shares,
                                        skip=skip, own=bool(own), last=bool(values)),
            out_shape=out if values else state_shape,
            in_specs=specs, out_specs=vmem(1)[0] if values else tuple(vmem(3)),
            scratch_shapes=scratch,
            compiler_params=pltpu.CompilerParams(vmem_limit_bytes=20 << 20),
            cost_estimate=pl.CostEstimate(
                flops=2_300_000 * count, bytes_accessed=6_000_000,
                transcendentals=1000 * count),
        )(meta, *inputs)

    state = attend(cat(window, others[0]), (1, 2), own=(latent_rows,))
    state = attend(near_flat, (3, 4), skip=2 * window.shape[0], state=state)
    answer = attend(far.reshape(near_flat.shape), (5, 6, 7, 8), state=state,
                    values=(absorb_value,))
    return (answer, arrived[None])


def solution(mesh):
    in_specs = (
        P(("group", "ctx"), ("head", "dec")),
        P(("group", "ctx"), None),
        P("group"),
        P(("group", "ctx"), None),
        P(("head", "dec"), None, None),
        P(("head", "dec"), None, None),
    )
    out_specs = (P(("group", "ctx"), ("head", "dec")), P(("group", "ctx", "dec"), None, None, None))
    return jax.shard_map(program, mesh=mesh, in_specs=in_specs, out_specs=out_specs, check_vma=False)
```
